1024 devices in a mesh: grp: 16 (over y, core), blk: 64 (over z, x).
Axes of the slice: x: 8, y: 8, z: 8, core: 2. Of those that a mesh axis runs over, the one named last changes fastest.
Arguments:
- child_field: bfloat16 [1048576, 384], P(('grp', 'blk')), may hold values from -6 to 6
- child_weight: bfloat16 [1048576], P(('grp', 'blk')), may hold values from 0.099609375 to 0.5
- child_slot: int32 [1048576], P(('grp', 'blk')), may hold values from 0 to 639, as said below
- send_list: int32 [1024, 640], P(('grp', 'blk')), may hold values from -1 to 255, as said below
- theta: float32 [128, 2048], P('grp', 'blk'), may hold values from 0.05 to 0.24
Outputs:
- corrected: float32 [128, 2048, 384], P('grp', 'blk')
The draws below stay inside these ranges and needn't reach their ends.
Inputs may be any that keep to these rules, and one draw needn't show every extreme that they name: `send_list`: row v lists, for each of its 5 nearby owners k = 0, 1, ... in turn, 128 slots: used slots first, each holding a distinct local parent number e of that owner, then -1 for unused slots; every device uses at least one slot for each nearby owner, and in every device's row one nearby owner has all 128 slots used. `child_slot`: A child's slot is k * 128 + position and is a used slot of its device's row of send_list.
All inputs are finite; a program needn't handle non-finite values.
Results may differ from the reference program's by a relative error of at most 0.0007.
Values sent between devices are 32-bit elements; how exact they have to be, the bound alone decides.
No kernel may reach another device: no remote copies, remote signals or barrier semaphores. Data moves between devices by JAX's collectives and lax.ppermute only.
A program may use at most 32 MiB of HBM per device.

```python
import math
import jax
import jax.numpy as jnp
from jax import lax

CC = 1024
PR = 8
PCOL = 32
HALF = 2
CAP = 128
CHANNELS = 384
NPR = 128
NPC = 2048
CHILDREN = 1048576
N_GRP = 16
N_BLK = 64


def slot_plan(key):
    base = jax.random.fold_in(key, 4099)
    keys = jax.random.split(base, 5)
    devices_all = N_GRP * N_BLK
    cells = PR * PCOL
    reach = 2 * HALF + 1
    upper = max(1, CAP // 4) + 1
    counts = jax.random.randint(keys[0], (devices_all, reach), 1, upper)
    fullest = jax.random.randint(keys[1], (devices_all,), 0, reach)
    owners = jnp.arange(reach)[None, :]
    counts = jnp.where(owners == fullest[:, None], CAP, counts).astype(jnp.int32)
    scores = jax.random.randint(keys[2], (devices_all, reach, cells), 0, 1 << 20) * cells + jnp.arange(cells)
    order = jnp.argsort(scores, axis=-1)[..., :CAP].astype(jnp.int32)
    used = jnp.arange(CAP)[None, None, :] < counts[..., None]
    lists = jnp.where(used, order, -1).reshape(devices_all, reach * CAP).astype(jnp.int32)
    target = jax.random.randint(keys[3], (devices_all, CC), 0, reach).astype(jnp.int32)
    limit = jnp.take_along_axis(counts, target, axis=1)
    picks = jax.random.randint(keys[4], (devices_all, CC), 0, 1 << 20) % limit
    slots = (target * CAP + picks).reshape(-1).astype(jnp.int32)
    return (lists, slots)


def draw_send_list(key, part):
    return slot_plan(key)[0]


def draw_child_slot(key, part):
    return slot_plan(key)[1]


def block_levels(own_key, dims, cuts, low, high):
    def one(position, shards_of):
        steps = jax.random.uniform(jax.random.fold_in(jax.random.fold_in(own_key, 6), position), (shards_of,), jnp.float32, low / len(cuts), high / len(cuts))
        return jnp.repeat(jnp.exp(steps), dims[position] // shards_of).reshape((-1,) + (1,) * (len(dims) - position - 1))

    gain = one(*cuts[0])
    for cut in cuts[1:]:
        gain = gain * one(*cut)
    return gain


def bell_draw(key, shape, width, most, cuts=(), held_as=jnp.bfloat16):
    entries = jax.random.normal(key, shape, jnp.float32) * width
    if len(cuts) > 0:
        entries = block_levels(key, shape, cuts, -0.22, 0.18) * entries
    return jnp.clip(entries, min=-most, max=most).astype(held_as)


def setup_inputs(seed: int = 0) -> dict:
    key_list = jax.random.split(jax.random.key(seed), 6)
    child_field = bell_draw(key_list[0], (CHILDREN, CHANNELS), 1.0, 6.0, ((0, 1024),))
    child_weight = jnp.clip(jnp.exp(math.log(0.5) - 1.6133518 * jax.random.uniform(key_list[1], (CHILDREN,), jnp.float32) ** block_levels(key_list[1], (CHILDREN,), ((0, 1024),), -0.2, 0.2)), 0.099609375, 0.5).astype(jnp.bfloat16)
    child_slot = draw_child_slot(jax.random.fold_in(key_list[5], 71), 0)
    send_list = draw_send_list(jax.random.fold_in(key_list[5], 71), 0)
    theta = jnp.clip(jnp.exp(math.log(0.24) - 1.5686159 * jax.random.uniform(key_list[4], (NPR, NPC), jnp.float32) ** block_levels(key_list[4], (NPR, NPC), ((0, 16), (1, 64)), -0.2, 0.2)), 0.05, 0.24)
    return {"child_field": child_field, "child_weight": child_weight, "child_slot": child_slot, "send_list": send_list, "theta": theta}


def reference(child_field, child_weight, child_slot, send_list, theta):
    cells = PR * PCOL
    fields = child_field.reshape(N_GRP, N_BLK * CC, CHANNELS)
    weights = child_weight.reshape(N_GRP, N_BLK * CC)
    slots = child_slot.reshape(N_GRP, N_BLK, CC).astype(jnp.int32)
    lists = send_list.reshape(N_GRP, N_BLK, (2 * HALF + 1) * CAP).astype(jnp.int32)

    def one_group(items):
        field, weight, slot, table = items
        entry = jnp.take_along_axis(table, slot, axis=1)
        block = jnp.arange(N_BLK, dtype=jnp.int32)[:, None]
        owner = (block + slot // CAP - HALF) % N_BLK
        parent = (owner * cells + entry).reshape(-1).astype(jnp.int32)
        terms = field.astype(jnp.float32) * weight.astype(jnp.float32)[:, None]
        sums = jax.ops.segment_sum(terms, parent, num_segments=N_BLK * cells)
        sums = sums.reshape(N_BLK, PR, PCOL, CHANNELS).transpose(1, 0, 2, 3)
        return sums.reshape(PR, N_BLK * PCOL, CHANNELS)

    restricted = lax.map(one_group, (fields, weights, slots, lists))
    restricted = restricted.reshape(N_GRP * PR, N_BLK * PCOL, CHANNELS)
    padded = jnp.pad(restricted, ((1, 1), (1, 1), (0, 0)))
    beside = padded[2:, 1:-1] + padded[:-2, 1:-1] + padded[1:-1, 2:] + padded[1:-1, :-2]
    return restricted + theta[:, :, None] * (beside - 4.0 * restricted)
```

```python
import functools

import jax
import jax.numpy as jnp
from jax import lax
from jax.experimental import pallas as pl
from jax.experimental.pallas import tpu as pltpu
from jax.sharding import PartitionSpec as P


PR = 8
PCOL = 32
CELLS = PR * PCOL
HALF = 2
REACH = 2 * HALF + 1
CAP = 128
LANES = 128
F32 = jnp.float32
BF16 = jnp.bfloat16

VMEM = pl.BlockSpec(memory_space=pltpu.VMEM)
SMEM = pl.BlockSpec(memory_space=pltpu.SMEM)


def shift(x, axis, by):
    size = lax.axis_size(axis)
    return lax.ppermute(x, axis, [(i, (i + by) % size) for i in range(size)])


def step(x, axis, by):
    size = lax.axis_size(axis)
    return lax.ppermute(x, axis, [(i, i + by) for i in range(size) if 0 <= i + by < size])


def swap(x, axis, first):
    size = lax.axis_size(axis)
    pairs = []
    for i in range(first, size - 1, 2):
        pairs += [(i, i + 1), (i + 1, i)]
    return lax.ppermute(x, axis, pairs)


def slot_sums(field, weight, slot, k):
    ids = k * CAP + lax.broadcasted_iota(jnp.int32, (CAP, slot.shape[1]), 0)
    matrix = jnp.where(ids == slot, weight, 0.0).astype(BF16)
    return jnp.dot(matrix, field, preferred_element_type=F32)


def spread(matrix, sums):
    high = sums.astype(BF16)
    low = (sums - high.astype(F32)).astype(BF16)
    both = jnp.dot(matrix, high, preferred_element_type=F32)
    return both + jnp.dot(matrix, low, preferred_element_type=F32)


def send_kernel(ks, field_ref, weight_ref, slot_ref, list_ref, *out_refs):
    for k, out_ref in zip(ks, out_refs):
        sums = slot_sums(field_ref[...], weight_ref[...], slot_ref[...], k)
        for j in range(sums.shape[1] // LANES):
            out_ref[j * CAP : (j + 1) * CAP, :] = sums[:, j * LANES : (j + 1) * LANES]
        row = list_ref[k : k + 1, :].astype(F32)
        out_ref[sums.shape[1] : sums.shape[1] + 8, :] = jnp.broadcast_to(row, (8, LANES))


def own_kernel(field_ref, weight_ref, slot_ref, list_ref, theta_ref, out_ref, wide_ref):
    sums = slot_sums(field_ref[...], weight_ref[...], slot_ref[...], HALF)
    row = list_ref[HALF : HALF + 1, :]
    matrix = jnp.where(lax.broadcasted_iota(jnp.int32, (CELLS, CAP), 0) == row, 1.0, 0.0).astype(BF16)
    out_ref[...] = spread(matrix, sums)
    here = lax.broadcasted_iota(jnp.int32, (PCOL, PCOL), 0) == lax.broadcasted_iota(jnp.int32, (PCOL, PCOL), 1)
    for r in range(PR):
        column = jnp.sum(jnp.where(here, theta_ref[r : r + 1, :], 0.0), axis=1, keepdims=True)
        wide_ref[r * PCOL : (r + 1) * PCOL, :] = jnp.broadcast_to(column, (PCOL, LANES))


def gather_kernel(odd_ref, own_ref, *refs):
    messages, (out_ref, chip_ref, side_ref, last_ref, first_ref) = refs[:-5], refs[-5:]
    channels = own_ref.shape[1]
    cells = lax.broadcasted_iota(jnp.int32, (CELLS, CAP), 0).astype(F32)
    for j in range(channels // LANES):
        total = own_ref[:, j * LANES : (j + 1) * LANES]
        for msg in messages:
            matrix = jnp.where(cells == msg[channels : channels + 1, :], 1.0, 0.0).astype(BF16)
            total = total + spread(matrix, msg[j * CAP : (j + 1) * CAP, :])
        out_ref[:, j * LANES : (j + 1) * LANES] = total
    odd = odd_ref[0]
    tail = (PR - 1) * PCOL
    chip_ref[...] = out_ref[pl.ds(pl.multiple_of((1 - odd) * tail, PCOL), PCOL), :]
    side_ref[...] = out_ref[pl.ds(pl.multiple_of(odd * tail, PCOL), PCOL), :]
    for r in range(PR):
        last_ref[r : r + 1, :] = out_ref[(r + 1) * PCOL - 1 : (r + 1) * PCOL, :]
        first_ref[r : r + 1, :] = out_ref[r * PCOL : r * PCOL + 1, :]


def final_kernel(odd_ref, own_ref, wide_ref, chip_ref, side_ref, left_ref, right_ref, out_ref):
    odd = odd_ref[0] == 1
    for r in range(PR):
        low, high = r * PCOL, (r + 1) * PCOL
        here = own_ref[low:high, :]
        if r == 0:
            above = jnp.where(odd, chip_ref[...], side_ref[...])
        else:
            above = own_ref[low - PCOL : low, :]
        if r == PR - 1:
            below = jnp.where(odd, side_ref[...], chip_ref[...])
        else:
            below = own_ref[high : high + PCOL, :]
        west = jnp.concatenate([left_ref[r : r + 1, :], here[:-1]], axis=0)
        east = jnp.concatenate([here[1:], right_ref[r : r + 1, :]], axis=0)
        factor = jnp.concatenate([wide_ref[low:high, :]] * (here.shape[1] // LANES), axis=1)
        out_ref[low:high, :] = here + factor * (below + above + east + west - 4.0 * here)


def struct(shape, dtype=F32):
    return jax.ShapeDtypeStruct(shape, dtype)


def call(kernel, outs, specs, flops):
    return pl.pallas_call(
        kernel,
        out_shape=outs,
        in_specs=specs,
        out_specs=jax.tree.map(lambda _: VMEM, outs),
        compiler_params=pltpu.CompilerParams(vmem_limit_bytes=16 * 1024 * 1024),
        cost_estimate=pl.CostEstimate(flops=flops, bytes_accessed=1000000, transcendentals=0),
    )


def body(child_field, child_weight, child_slot, send_list, theta):
    children, channels = child_field.shape
    weight = child_weight.astype(F32).reshape(1, children)
    slot = child_slot.reshape(1, children)
    listed = send_list.reshape(REACH, CAP)
    odd = (lax.axis_index("grp") % 2).reshape(1).astype(jnp.int32)
    message = struct((channels + 8, LANES))
    work = 2 * CAP * children * channels

    def sends(ks):
        kernel = functools.partial(send_kernel, ks)
        outs = [message] * len(ks)
        return call(kernel, outs, [VMEM] * 4, work * len(ks))(child_field, weight, slot, listed)

    arrived = []
    for k in (4, 3, 1, 0):
        (msg,) = sends((k,))
        arrived.append(shift(msg, "blk", k - HALF))
    own, wide = call(own_kernel, [struct((CELLS, channels)), struct((CELLS, LANES))], [VMEM] * 5, 2 * work)(
        child_field, weight, slot, listed, theta
    )
    outs = [struct((CELLS, channels))] + [struct((PCOL, channels))] * 2 + [struct((PR, channels))] * 2
    restricted, chip, side, last, first = call(gather_kernel, outs, [SMEM] + [VMEM] * 5, work)(odd, own, *arrived)
    side = swap(side, "grp", 1)
    left = step(last, "blk", 1)
    right = step(first, "blk", -1)
    chip = swap(chip, "grp", 0)
    out = call(final_kernel, struct((CELLS, channels)), [SMEM] + [VMEM] * 6, work)(
        odd, restricted, wide, chip, side, left, right
    )
    return out.reshape(PR, PCOL, channels)


def solution(mesh):
    return jax.shard_map(
        body,
        mesh=mesh,
        in_specs=(
            P(("grp", "blk"), None),
            P(("grp", "blk")),
            P(("grp", "blk")),
            P(("grp", "blk"), None),
            P("grp", "blk"),
        ),
        out_specs=P("grp", "blk", None),
        check_vma=False,
    )
```

```python
import functools

import jax
import jax.numpy as jnp
from jax import lax
from jax.experimental import pallas as pl
from jax.experimental.pallas import tpu as pltpu
from jax.sharding import PartitionSpec as P


PR = 8
PCOL = 32
CELLS = PR * PCOL
HALF = 2
CAP = 128
LANES = 128
F32 = jnp.float32
BF16 = jnp.bfloat16

VMEM = pl.BlockSpec(memory_space=pltpu.VMEM)
SMEM = pl.BlockSpec(memory_space=pltpu.SMEM)


def swap_open(x, axis, first):
    size = lax.axis_size(axis)
    pairs = []
    for i in range(first, size - 1, 2):
        pairs += [(i, i + 1), (i + 1, i)]
    return lax.ppermute(x, axis, pairs)


def iota(shape, dim):
    return lax.broadcasted_iota(jnp.int32, shape, dim)


def slot_sums(weight_ref, slot_ref, field_ref, k):
    ids = k * CAP + iota((CAP, LANES), 0)
    weight, slot = weight_ref[...].astype(F32), slot_ref[...]
    blocks = [
        jnp.where(ids == slot[j : j + 1, :], weight[j : j + 1, :], 0.0).astype(BF16) for j in range(slot.shape[0])
    ]
    return jnp.dot(jnp.concatenate(blocks, axis=1), field_ref[...], preferred_element_type=F32)


def one_hot(ids, row):
    return jnp.where(ids == row, 1.0, 0.0).astype(BF16)


def spread(matrix, sums):
    high = sums.astype(BF16)
    low = (sums - high.astype(F32)).astype(BF16)
    both = jnp.dot(matrix, high, preferred_element_type=F32)
    return both + jnp.dot(matrix, low, preferred_element_type=F32)


def send_kernel(choose, blk_ref, weight_ref, slot_ref, field_ref, list_ref, out_ref):
    k = choose(blk_ref[0])
    at = pl.ds(pl.multiple_of(k * CAP, CAP), CAP)
    sums = slot_sums(weight_ref, slot_ref, field_ref, k)
    channels = sums.shape[1]
    for j in range(channels // LANES):
        out_ref[j * CAP : (j + 1) * CAP, :] = sums[:, j * LANES : (j + 1) * LANES]
    out_ref[channels : channels + 8, :] = jnp.broadcast_to(list_ref[:, at].astype(F32), (8, LANES))


def own_kernel(weight_ref, slot_ref, field_ref, list_ref, theta_ref, out_ref, wide_ref):
    mine = slice(HALF * CAP, (HALF + 1) * CAP)
    sums = slot_sums(weight_ref, slot_ref, field_ref, HALF)
    out_ref[...] = spread(one_hot(iota((CELLS, CAP), 0), list_ref[:, mine]), sums)
    here = iota((PCOL, PCOL), 0) == iota((PCOL, PCOL), 1)
    for r in range(PR):
        column = jnp.sum(jnp.where(here, theta_ref[r : r + 1, :], 0.0), axis=1, keepdims=True)
        wide_ref[r * PCOL : (r + 1) * PCOL, :] = jnp.broadcast_to(column, (PCOL, LANES))


def gather_kernel(grp_ref, own_ref, *refs):
    messages, (out_ref, chip_ref, side_ref, last_ref, first_ref) = refs[:-5], refs[-5:]
    channels = own_ref.shape[1]
    cells = iota((CELLS, CAP), 0).astype(F32)
    matrices = [one_hot(cells, msg[channels : channels + 1, :]) for msg in messages]
    for j in range(channels // LANES):
        lanes = slice(j * LANES, (j + 1) * LANES)
        total = own_ref[:, lanes]
        for matrix, msg in zip(matrices, messages):
            total = total + spread(matrix, msg[j * CAP : (j + 1) * CAP, :])
        out_ref[:, lanes] = total
    odd = grp_ref[0] % 2
    tail = (PR - 1) * PCOL
    chip_ref[...] = out_ref[pl.ds(pl.multiple_of((1 - odd) * tail, PCOL), PCOL), :]
    side_ref[...] = out_ref[pl.ds(pl.multiple_of(odd * tail, PCOL), PCOL), :]
    for r in range(PR):
        last_ref[r : r + 1, :] = out_ref[(r + 1) * PCOL - 1 : (r + 1) * PCOL, :]
        first_ref[r : r + 1, :] = out_ref[r * PCOL : r * PCOL + 1, :]


def final_kernel(grp_ref, own_ref, wide_ref, chip_ref, side_ref, left_ref, right_ref, out_ref):
    odd = grp_ref[0] % 2 == 1
    for r in range(PR):
        low, high = r * PCOL, (r + 1) * PCOL
        here = own_ref[low:high, :]
        if r == 0:
            above = jnp.where(odd, chip_ref[...], side_ref[...])
        else:
            above = own_ref[low - PCOL : low, :]
        if r == PR - 1:
            below = jnp.where(odd, side_ref[...], chip_ref[...])
        else:
            below = own_ref[high : high + PCOL, :]
        west = jnp.concatenate([left_ref[r : r + 1, :], here[:-1]], axis=0)
        east = jnp.concatenate([here[1:], right_ref[r : r + 1, :]], axis=0)
        factor = jnp.concatenate([wide_ref[low:high, :]] * (here.shape[1] // LANES), axis=1)
        out_ref[low:high, :] = here + factor * (below + above + east + west - 4.0 * here)


def struct(shape, dtype=F32):
    return jax.ShapeDtypeStruct(shape, dtype)


def call(kernel, outs, specs, flops, scratch=(), grant=8):
    return pl.pallas_call(
        kernel,
        out_shape=outs,
        in_specs=specs,
        out_specs=jax.tree.map(lambda _: VMEM, outs),
        scratch_shapes=scratch,
        compiler_params=pltpu.CompilerParams(vmem_limit_bytes=grant * 1024 * 1024),
        cost_estimate=pl.CostEstimate(flops=flops, bytes_accessed=1000000, transcendentals=0),
    )


def body(child_field, child_weight, child_slot, send_list, theta):
    children, channels = child_field.shape
    size = lax.axis_size("blk")
    blk = lax.axis_index("blk").reshape(1).astype(jnp.int32)
    grp = lax.axis_index("grp").reshape(1).astype(jnp.int32)
    weight = child_weight.reshape(children // LANES, LANES)
    slot = child_slot.reshape(children // LANES, LANES)
    work = 2 * CAP * children * channels
    message = struct((channels + 8, LANES))

    def trade(choose, pairs):
        kernel = functools.partial(send_kernel, choose)
        msg = call(kernel, message, [SMEM] + [VMEM] * 4, work)(blk, weight, slot, child_field, send_list)
        return lax.ppermute(msg, "blk", pairs)

    last = size - 1
    down = [(i, i - 1) for i in range(1, last)]
    across = [(i, i + 1) for i in range(1, last - 1)] + [(last, 0), (0, last)]
    rest = [(0, 1), (last - 1, last), (last, last - 1)]
    m1 = trade(lambda i: 1 + 0 * i, down)
    p2 = trade(lambda i: 4 + 0 * i, [(i, (i + 2) % size) for i in range(size)])
    f1 = trade(lambda i: jnp.where(i == 0, 1, 3), across)
    m2 = trade(lambda i: 0 * i, [(i, (i - 2) % size) for i in range(size)])
    g1 = trade(lambda i: jnp.where(i == last, 1, 3), rest)
    own, wide = call(
        own_kernel, [struct((CELLS, channels)), struct((CELLS, LANES))], [VMEM] * 5, 2 * work
    )(weight, slot, child_field, send_list, theta)
    row, narrow = struct((PCOL, channels)), struct((PR, channels))
    restricted, chip, side, tail, head = call(
        gather_kernel, [struct((CELLS, channels)), row, row, narrow, narrow], [SMEM] + [VMEM] * 6, work
    )(grp, own, m1, p2, f1, m2, g1)
    side = swap_open(side, "grp", 1)
    left = lax.ppermute(tail, "blk", [(i, i + 1) for i in range(last)])
    right = lax.ppermute(head, "blk", [(i + 1, i) for i in range(last)])
    chip = swap_open(chip, "grp", 0)
    out = call(final_kernel, struct((CELLS, channels)), [SMEM] + [VMEM] * 6, work)(
        grp, restricted, wide, chip, side, left, right
    )
    return out.reshape(PR, PCOL, channels)


def solution(mesh):
    return jax.shard_map(
        body,
        mesh=mesh,
        in_specs=(
            P(("grp", "blk"), None),
            P(("grp", "blk")),
            P(("grp", "blk")),
            P(("grp", "blk"), None),
            P("grp", "blk"),
        ),
        out_specs=P("grp", "blk", None),
        check_vma=False,
    )
```

```python
import functools

import jax
import jax.numpy as jnp
from jax import lax
from jax.experimental import pallas as pl
from jax.experimental.pallas import tpu as pltpu
from jax.sharding import PartitionSpec as P


PR = 8
PCOL = 32
CELLS = PR * PCOL
HALF = 2
CAP = 128
LANES = 128
F32 = jnp.float32
BF16 = jnp.bfloat16

VMEM = pl.BlockSpec(memory_space=pltpu.VMEM)
SMEM = pl.BlockSpec(memory_space=pltpu.SMEM)


def swap_open(x, axis, first):
    size = lax.axis_size(axis)
    pairs = []
    for i in range(first, size - 1, 2):
        pairs += [(i, i + 1), (i + 1, i)]
    return lax.ppermute(x, axis, pairs)


def iota(shape, dim):
    return lax.broadcasted_iota(jnp.int32, shape, dim)


def slot_sums(weight_ref, slot_ref, field_ref, k):
    ids = k * CAP + iota((CAP, LANES), 0)
    weight, slot = weight_ref[...].astype(F32), slot_ref[...]
    blocks = [
        jnp.where(ids == slot[j : j + 1, :], weight[j : j + 1, :], 0.0).astype(BF16) for j in range(slot.shape[0])
    ]
    return jnp.dot(jnp.concatenate(blocks, axis=1), field_ref[...], preferred_element_type=F32)


def one_hot(ids, row):
    return jnp.where(ids == row, 1.0, 0.0).astype(BF16)


def spread(matrix, sums):
    high = sums.astype(BF16)
    low = (sums - high.astype(F32)).astype(BF16)
    both = jnp.dot(matrix, high, preferred_element_type=F32)
    return both + jnp.dot(matrix, low, preferred_element_type=F32)


def send_kernel(choose, blk_ref, weight_ref, slot_ref, field_ref, list_ref, out_ref):
    k = choose(blk_ref[0])
    at = pl.ds(pl.multiple_of(k * CAP, CAP), CAP)
    sums = slot_sums(weight_ref, slot_ref, field_ref, k)
    channels = sums.shape[1]
    for j in range(channels // LANES):
        out_ref[j * CAP : (j + 1) * CAP, :] = sums[:, j * LANES : (j + 1) * LANES]
    out_ref[channels : channels + 8, :] = jnp.broadcast_to(list_ref[:, at].astype(F32), (8, LANES))


def own_kernel(weight_ref, slot_ref, field_ref, list_ref, theta_ref, out_ref, wide_ref):
    mine = slice(HALF * CAP, (HALF + 1) * CAP)
    sums = slot_sums(weight_ref, slot_ref, field_ref, HALF)
    out_ref[...] = spread(one_hot(iota((CELLS, CAP), 0), list_ref[:, mine]), sums)
    here = iota((PCOL, PCOL), 0) == iota((PCOL, PCOL), 1)
    for r in range(PR):
        column = jnp.sum(jnp.where(here, theta_ref[r : r + 1, :], 0.0), axis=1, keepdims=True)
        wide_ref[r * PCOL : (r + 1) * PCOL, :] = jnp.broadcast_to(column, (PCOL, LANES))


def gather_kernel(grp_ref, own_ref, *refs):
    messages, (out_ref, chip_ref, side_ref, last_ref, first_ref) = refs[:-5], refs[-5:]
    channels = own_ref.shape[1]
    cells = iota((CELLS, CAP), 0).astype(F32)
    matrices = [one_hot(cells, msg[channels : channels + 1, :]) for msg in messages]
    for j in range(channels // LANES):
        lanes = slice(j * LANES, (j + 1) * LANES)
        total = own_ref[:, lanes]
        for matrix, msg in zip(matrices, messages):
            total = total + spread(matrix, msg[j * CAP : (j + 1) * CAP, :])
        out_ref[:, lanes] = total
    odd = grp_ref[0] % 2
    tail = (PR - 1) * PCOL
    chip_ref[...] = out_ref[pl.ds(pl.multiple_of((1 - odd) * tail, PCOL), PCOL), :]
    side_ref[...] = out_ref[pl.ds(pl.multiple_of(odd * tail, PCOL), PCOL), :]
    for r in range(PR):
        last_ref[r : r + 1, :] = out_ref[(r + 1) * PCOL - 1 : (r + 1) * PCOL, :]
        first_ref[r : r + 1, :] = out_ref[r * PCOL : r * PCOL + 1, :]


def final_kernel(grp_ref, own_ref, wide_ref, chip_ref, side_ref, left_ref, right_ref, out_ref):
    odd = grp_ref[0] % 2 == 1
    for r in range(PR):
        low, high = r * PCOL, (r + 1) * PCOL
        here = own_ref[low:high, :]
        if r == 0:
            above = jnp.where(odd, chip_ref[...], side_ref[...])
        else:
            above = own_ref[low - PCOL : low, :]
        if r == PR - 1:
            below = jnp.where(odd, side_ref[...], chip_ref[...])
        else:
            below = own_ref[high : high + PCOL, :]
        west = jnp.concatenate([left_ref[r : r + 1, :], here[:-1]], axis=0)
        east = jnp.concatenate([here[1:], right_ref[r : r + 1, :]], axis=0)
        factor = jnp.concatenate([wide_ref[low:high, :]] * (here.shape[1] // LANES), axis=1)
        out_ref[low:high, :] = here + factor * (below + above + east + west - 4.0 * here)


def struct(shape, dtype=F32):
    return jax.ShapeDtypeStruct(shape, dtype)


def call(kernel, outs, specs, flops, scratch=(), grant=8):
    return pl.pallas_call(
        kernel,
        out_shape=outs,
        in_specs=specs,
        out_specs=jax.tree.map(lambda _: VMEM, outs),
        scratch_shapes=scratch,
        compiler_params=pltpu.CompilerParams(vmem_limit_bytes=grant * 1024 * 1024),
        cost_estimate=pl.CostEstimate(flops=flops, bytes_accessed=1000000, transcendentals=0),
    )


def body(child_field, child_weight, child_slot, send_list, theta):
    children, channels = child_field.shape
    size = lax.axis_size("blk")
    blk = lax.axis_index("blk").reshape(1).astype(jnp.int32)
    grp = lax.axis_index("grp").reshape(1).astype(jnp.int32)
    weight = child_weight.reshape(children // LANES, LANES)
    slot = child_slot.reshape(children // LANES, LANES)
    work = 2 * CAP * children * channels
    message = struct((channels + 8, LANES))

    def trade(choose, pairs):
        kernel = functools.partial(send_kernel, choose)
        msg = call(kernel, message, [SMEM] + [VMEM] * 4, work)(blk, weight, slot, child_field, send_list)
        return lax.ppermute(msg, "blk", pairs)

    last = size - 1
    down = [(i, i - 1) for i in range(1, last - 1)]
    across = [(i, i + 1) for i in (*range(1, last - 3), last - 2)] + [(last, 0), (0, last), (last - 1, last - 2)]
    rest = [(0, 1), (last - 3, last - 2), (last - 1, last), (last, last - 1)]
    p2 = trade(lambda i: 4 + 0 * i, [(i, (i + 2) % size) for i in range(size)])
    m1 = trade(lambda i: 1 + 0 * i, down)
    f1 = trade(lambda i: jnp.where((i == 0) | (i == last - 1), 1, 3), across)
    m2 = trade(lambda i: 0 * i, [(i, (i - 2) % size) for i in range(size)])
    g1 = trade(lambda i: jnp.where(i == last, 1, 3), rest)
    own, wide = call(
        own_kernel, [struct((CELLS, channels)), struct((CELLS, LANES))], [VMEM] * 5, 2 * work
    )(weight, slot, child_field, send_list, theta)
    row, narrow = struct((PCOL, channels)), struct((PR, channels))
    restricted, chip, side, tail, head = call(
        gather_kernel, [struct((CELLS, channels)), row, row, narrow, narrow], [SMEM] + [VMEM] * 6, work
    )(grp, own, m1, p2, f1, m2, g1)
    side = swap_open(side, "grp", 1)
    left = lax.ppermute(tail, "blk", [(i, i + 1) for i in range(last)])
    right = lax.ppermute(head, "blk", [(i + 1, i) for i in range(last)])
    chip = swap_open(chip, "grp", 0)
    out = call(final_kernel, struct((CELLS, channels)), [SMEM] + [VMEM] * 6, work)(
        grp, restricted, wide, chip, side, left, right
    )
    return out.reshape(PR, PCOL, channels)


def solution(mesh):
    return jax.shard_map(
        body,
        mesh=mesh,
        in_specs=(
            P(("grp", "blk"), None),
            P(("grp", "blk")),
            P(("grp", "blk")),
            P(("grp", "blk"), None),
            P("grp", "blk"),
        ),
        out_specs=P("grp", "blk", None),
        check_vma=False,
    )
```
